32 devices in a mesh: src: 8 (over z, x), rcv: 4 (over y, core).
Axes of the slice: x: 2, y: 2, z: 4, core: 2. Of those that a mesh axis runs over, the one named last changes fastest.
Arguments:
- traces: bfloat16 [2, 2, 2048, 2048], P(None, None, 'src', 'rcv'), may hold values from -8 to 8
- wavelet: float32 [2, 2], replicated, may hold values from -0.3 to 0.3
Outputs:
- coeffs: float32 [2, 2, 2048, 2048], P(None, None, 'src', 'rcv')
- norms: float32 [2, 2], replicated
The draws below stay inside these ranges and needn't reach their ends.
All inputs are finite; a program needn't handle non-finite values.
Results may differ from the reference program's by a relative error of at most 0.006.
Values may be sent and summed in bfloat16 or wider, within the bound.
A program may use at most 128 MiB of HBM per device.

```python
import math
import jax
import jax.numpy as jnp
from jax import lax

N = 2048
NF = 2
ITERS = 2


def draw_traces(key, part):
    values = jax.random.normal(jax.random.fold_in(key, 11), (NF, 2, N, N), jnp.float32)
    position = jnp.arange(N, dtype=jnp.float32) / N
    trend = jnp.exp(-math.log(4.0) * position)[None, None, :, None]
    values = values * trend * 1.3
    return jnp.clip(values, -8.0, 8.0).astype(jnp.bfloat16)


def setup_inputs(seed: int = 0) -> dict:
    seeds = jax.random.split(jax.random.key(seed), 3)
    traces = draw_traces(jax.random.fold_in(seeds[2], 71), 0)
    wavelet = jnp.clip(jax.random.uniform(seeds[1], (NF, 2), jnp.float32, -0.3, 0.3), -0.3, 0.3)
    return dict(traces=traces, wavelet=wavelet)


step_length = 0.4
shrink_fraction = 0.2

def table_block(offset, height, second, breadth, length, direction):
    left_index = offset + jnp.arange(height, dtype=jnp.int32)
    right_index = second + jnp.arange(breadth, dtype=jnp.int32)
    phase = left_index[:, None] * right_index[None, :] % length
    angle = phase.astype(jnp.float32) * (2.0 * math.pi / length)
    scale = 1.0 / math.sqrt(length)
    return jnp.stack([jnp.cos(angle) * scale, direction * (jnp.sin(angle) * scale)]).astype(jnp.bfloat16)

def rounded(values):
    return lax.optimization_barrier(values.astype(jnp.bfloat16)).astype(jnp.float32)

def matmul_high(left_side, right_side):
    return jnp.matmul(left_side, right_side, precision=lax.Precision.HIGHEST)

def complex_matmul(left_side, right_side):
    left_re = left_side[..., 0, :, :]
    left_im = left_side[..., 1, :, :]
    right_re = right_side[..., 0, :, :]
    right_im = right_side[..., 1, :, :]
    real_part = matmul_high(left_re, right_re) - matmul_high(left_im, right_im)
    imag_part = matmul_high(left_re, right_im) + matmul_high(left_im, right_re)
    return jnp.stack([real_part, imag_part], axis=-3)

def complex_scale(real_part, imag_part, values):
    return jnp.stack([real_part * values[:, 0] - imag_part * values[:, 1], real_part * values[:, 1] + imag_part * values[:, 0]], axis=1)

def reference(traces, wavelet):
    extent = traces.shape[-1]
    forward = table_block(0, extent, 0, extent, extent, -1.0).astype(jnp.float32)
    inverse = table_block(0, extent, 0, extent, extent, 1.0).astype(jnp.float32)
    traces_f = traces.astype(jnp.float32)
    root_scale = 1.0 / math.sqrt(extent)
    wave_re = (wavelet[:, 0] * root_scale)[:, None, None]
    wave_im = (wavelet[:, 1] * root_scale)[:, None, None]
    traces_adj = jnp.stack([jnp.swapaxes(traces_f[:, 0], 1, 2), -jnp.swapaxes(traces_f[:, 1], 1, 2)], axis=1)
    coeffs = jnp.zeros(traces_f.shape, jnp.float32)
    norm_list = []
    for iteration in range(ITERS):
        if iteration == 0:
            misfit = traces_f
        else:
            halfway = rounded(complex_matmul(inverse, rounded(coeffs)))
            model = rounded(complex_matmul(halfway, inverse))
            product = complex_matmul(model, traces_f)
            misfit = traces_f - model + complex_scale(wave_re, wave_im, product)
        norm_list.append(jnp.sqrt(lax.optimization_barrier(jnp.sum(misfit * misfit, axis=(1, 2, 3)))))
        misfit_half = rounded(misfit)
        back_term = complex_matmul(misfit_half, traces_adj)
        gradient = misfit_half - complex_scale(wave_re, -wave_im, back_term)
        transformed = rounded(complex_matmul(rounded(gradient), forward))
        spectrum = complex_matmul(forward, transformed)
        trial = coeffs + step_length * spectrum
        magnitude = jnp.sqrt(trial[:, 0] * trial[:, 0] + trial[:, 1] * trial[:, 1])
        level = shrink_fraction * lax.optimization_barrier(jnp.max(magnitude, axis=(1, 2)))[:, None, None]
        factor = jnp.maximum(1.0 - level / jnp.maximum(magnitude, level), 0.0)
        coeffs = trial * factor[:, None]
    return (coeffs, jnp.stack(norm_list))
```

```python
import functools
import math

import jax
import jax.numpy as jnp
from jax import lax
from jax.experimental import pallas as pl
from jax.experimental.pallas import tpu as pltpu
from jax.sharding import PartitionSpec as P

ITERS = 2
CORES = 2
MESH = pl.DeviceIdType.MESH

step_length = 0.4
shrink_fraction = 0.2


def exchange_kernel(members, whole, x_ref, out_ref, send_sem, recv_sem, own_sem):
    count, me, device = members()
    barrier = pltpu.get_barrier_semaphore()
    for step in range(1, count):
        pl.semaphore_signal(
            barrier, inc=1, device_id=device(lax.rem(me + step, count)), device_id_type=MESH
        )
    pl.semaphore_wait(barrier, count - 1)
    own = pltpu.make_async_copy(x_ref if whole else x_ref.at[me], out_ref.at[me], own_sem)
    own.start()
    sends = []
    for step in range(1, count):
        peer = lax.rem(me + step, count)
        copy = pltpu.make_async_remote_copy(
            src_ref=x_ref if whole else x_ref.at[peer],
            dst_ref=out_ref.at[me],
            send_sem=send_sem.at[step],
            recv_sem=recv_sem.at[step],
            device_id=device(peer),
            device_id_type=MESH,
        )
        copy.start()
        sends.append(copy)
    own.wait()
    for step in range(1, count):
        origin = lax.rem(me - step + count, count)
        pltpu.make_async_remote_copy(
            src_ref=out_ref.at[origin],
            dst_ref=out_ref.at[origin],
            send_sem=send_sem.at[step],
            recv_sem=recv_sem.at[step],
            device_id=device(origin),
            device_id_type=MESH,
        ).wait_recv()
    for copy in sends:
        copy.wait_send()


def exchange(x, members, count, ident, whole=False):
    shape = (count,) + x.shape if whole else x.shape
    return pl.pallas_call(
        functools.partial(exchange_kernel, members, whole),
        out_shape=jax.ShapeDtypeStruct(shape, x.dtype),
        in_specs=[pl.BlockSpec(memory_space=pltpu.VMEM)],
        out_specs=pl.BlockSpec(memory_space=pltpu.VMEM),
        scratch_shapes=[
            pltpu.SemaphoreType.DMA((count,)),
            pltpu.SemaphoreType.DMA((count,)),
            pltpu.SemaphoreType.DMA,
        ],
        compiler_params=pltpu.CompilerParams(collective_id=ident, has_side_effects=True),
    )(x)


def gather_kernel(nz, ny, nf, x_ref, out_ref, own_sem, swap_sem, link_sem, core_sem, send_sem):
    src, rcv = lax.axis_index("src"), lax.axis_index("rcv")
    z, f = src // nf, lax.rem(src, nf)
    y, c = rcv // CORES, lax.rem(rcv, CORES)
    height, width = x_ref.shape[2], x_ref.shape[3]

    def device(zz, ff, yy, cc):
        return (zz * nf + ff, yy * CORES + cc)

    def block(zz, ff, yy, cc):
        top = pl.multiple_of((zz * nf + ff) * height, height)
        left = pl.multiple_of((yy * CORES + cc) * width, width)
        return out_ref.at[:, pl.ds(top, height), pl.ds(left, width)]

    z_peers = [lax.rem(z + d, nz) for d in range(1, nz)]
    y_peers = [lax.rem(y + e, ny) for e in range(1, ny)]
    f_peers = [lax.rem(f + g, nf) for g in range(1, nf)]
    other = 1 - c

    barrier = pltpu.get_barrier_semaphore()
    targets = [device(zz, f, y, c) for zz in z_peers]
    targets += [device(z, f, yy, c) for yy in y_peers]
    targets += [device(z, ff, y, c) for ff in f_peers]
    targets += [device(z, f, y, other)]
    for target in targets:
        pl.semaphore_signal(barrier, inc=1, device_id=target, device_id_type=MESH)
    pl.semaphore_wait(barrier, len(targets))

    sends = []

    def push(source, place, semaphore, target):
        copy = pltpu.make_async_remote_copy(
            src_ref=source,
            dst_ref=place,
            send_sem=send_sem.at[len(sends)],
            recv_sem=semaphore,
            device_id=target,
            device_id_type=MESH,
        )
        copy.start()
        sends.append(copy)

    def await_block(place, semaphore):
        pltpu.make_async_remote_copy(
            src_ref=place,
            dst_ref=place,
            send_sem=send_sem.at[0],
            recv_sem=semaphore,
            device_id=device(z, f, y, other),
            device_id_type=MESH,
        ).wait_recv()

    def across(zz, ff, yy):
        here = block(zz, ff, yy, c)
        push(here, here, core_sem.at[zz, ff, yy], device(z, f, y, other))

    def along_z(ff, yy):
        here = block(z, ff, yy, c)
        for zz in z_peers:
            push(here, here, link_sem.at[z, ff, yy], device(zz, f, y, c))

    def along_y(zz, ff):
        here = block(zz, ff, y, c)
        for yy in y_peers:
            push(here, here, link_sem.at[zz, ff, y], device(z, f, yy, c))

    for step, ff in enumerate(f_peers):
        push(x_ref.at[ff], block(z, f, y, c), swap_sem.at[step], device(z, ff, y, c))
    own = pltpu.make_async_copy(x_ref.at[f], block(z, f, y, c), own_sem)
    own.start()
    own.wait()
    for step in range(nf - 1):
        origin = lax.rem(f - 1 - step + nf, nf)
        await_block(block(z, origin, y, c), swap_sem.at[step])

    for ff in range(nf):
        if ff % 2 == 0:
            along_z(ff, y)
        else:
            along_y(z, ff)
    for ff in range(nf):
        across(z, ff, y)
    for ff in range(nf):
        if ff % 2 == 0:
            along_y(z, ff)
        else:
            along_z(ff, y)
    for ff in range(1, nf, 2):
        for yy in y_peers:
            await_block(block(z, ff, yy, c), link_sem.at[z, ff, yy])
            along_z(ff, yy)
            across(z, ff, yy)
    for ff in range(0, nf, 2):
        for zz in z_peers:
            await_block(block(zz, ff, y, c), link_sem.at[zz, ff, y])
            along_y(zz, ff)
            across(zz, ff, y)
    for ff in range(0, nf, 2):
        for yy in y_peers:
            await_block(block(z, ff, yy, c), link_sem.at[z, ff, yy])
            across(z, ff, yy)
    for ff in range(1, nf, 2):
        for zz in z_peers:
            await_block(block(zz, ff, y, c), link_sem.at[zz, ff, y])
            across(zz, ff, y)
    for ff in range(nf):
        for zz in z_peers:
            for yy in y_peers:
                await_block(block(zz, ff, yy, c), link_sem.at[zz, ff, yy])
                across(zz, ff, yy)
    for ff in range(nf):
        for zz in range(nz):
            for yy in range(ny):
                await_block(block(zz, ff, yy, other), core_sem.at[zz, ff, yy])
    for copy in sends:
        copy.wait_send()


def gather(traces, nz, ny, nf, extent):
    even, odd = (nf + 1) // 2, nf // 2
    total = (nf - 1) + nf * nz * ny
    total += even * ((nz - 1) + nz * (ny - 1)) + odd * ((ny - 1) + ny * (nz - 1))
    return pl.pallas_call(
        functools.partial(gather_kernel, nz, ny, nf),
        out_shape=jax.ShapeDtypeStruct((2, extent, extent), traces.dtype),
        in_specs=[pl.BlockSpec(memory_space=pltpu.VMEM)],
        out_specs=pl.BlockSpec(memory_space=pl.ANY),
        scratch_shapes=[
            pltpu.SemaphoreType.DMA,
            pltpu.SemaphoreType.DMA((nf,)),
            pltpu.SemaphoreType.DMA((nz, nf, ny)),
            pltpu.SemaphoreType.DMA((nz, nf, ny)),
            pltpu.SemaphoreType.DMA((total + nf * (nz + ny),)),
        ],
        compiler_params=pltpu.CompilerParams(collective_id=0, has_side_effects=True),
    )(traces)


def tables(extent):
    low = 1 << (extent.bit_length() // 2)
    while extent % low:
        low //= 2
    row = jnp.arange(extent, dtype=jnp.int32)

    def parts(column, scale):
        phase = row[:, None] * column[None, :] % extent
        angle = phase.astype(jnp.float32) * (2.0 * math.pi / extent)
        return lax.optimization_barrier((jnp.cos(angle) * scale, jnp.sin(angle) * scale))

    cos_low, sin_low = parts(jnp.arange(low, dtype=jnp.int32), 1.0)
    cos_high, sin_high = parts(
        jnp.arange(extent // low, dtype=jnp.int32) * low, 1.0 / math.sqrt(extent)
    )
    cos_high, sin_high = jnp.repeat(cos_high, low, 1), jnp.repeat(sin_high, low, 1)
    cos_low = jnp.tile(cos_low, (1, extent // low))
    sin_low = jnp.tile(sin_low, (1, extent // low))
    cosine = (cos_high * cos_low - sin_high * sin_low).astype(jnp.bfloat16)
    sine = (sin_high * cos_low + cos_high * sin_low).astype(jnp.bfloat16)
    return lax.optimization_barrier((cosine, sine))


def dot(left, right, pattern="mn,nc->mc"):
    return jnp.einsum(pattern, left, right, preferred_element_type=jnp.float32)


def per_device(nsrc, nrcv, traces, wavelet):
    nf, extent = traces.shape[0], traces.shape[2] * nsrc
    nz, ny = nsrc // nf, nrcv // CORES
    group = nz * nrcv
    part = extent // group
    src, rcv = lax.axis_index("src"), lax.axis_index("rcv")
    f = lax.rem(src, nf)
    place = rcv * nz + src // nf

    def same_frequency():
        src, rcv = lax.axis_index("src"), lax.axis_index("rcv")
        f = lax.rem(src, nf)
        return group, rcv * nz + src // nf, lambda i: (lax.rem(i, nz) * nf + f, i // nz)

    def same_column():
        rcv = lax.axis_index("rcv")
        return nsrc, lax.axis_index("src"), lambda i: (i, rcv)

    def everyone():
        me = lax.axis_index("src") * nrcv + lax.axis_index("rcv")
        return nsrc * nrcv, me, lambda i: (i // nrcv, lax.rem(i, nrcv))

    root_scale = 1.0 / math.sqrt(extent)
    wave = lax.dynamic_slice_in_dim(wavelet, f, 1, 0)[0] * root_scale
    wave_re, wave_im = wave[0], wave[1]

    cosine, sine = tables(extent)
    data = gather(traces, nz, ny, nf, extent)
    data_re, data_im = data[0], data[1]
    rows = lax.dynamic_slice_in_dim(data, place * part, part, 1)

    def rows_times(left, first, second, pattern="mn,nc->mc"):
        stacked = left.reshape(2 * part, extent)
        a = dot(stacked, first, pattern).reshape(2, part, extent)
        b = dot(stacked, second, pattern).reshape(2, part, extent)
        return a[0], a[1], b[0], b[1]

    def times_columns(right):
        a = dot(cosine, right).reshape(extent, 2, part)
        b = dot(sine, right).reshape(extent, 2, part)
        return a[:, 0], a[:, 1], b[:, 0], b[:, 1]

    coeffs_re = jnp.zeros((extent, part), jnp.float32)
    coeffs_im = coeffs_re
    norm_list = []
    for iteration in range(ITERS):
        if iteration == 0:
            misfit = rows.astype(jnp.float32)
        else:
            stacked = jnp.concatenate([coeffs_re, coeffs_im], 1).astype(jnp.bfloat16)
            re_c, im_c, re_s, im_s = times_columns(stacked)
            halfway = jnp.concatenate([re_c - im_s, im_c + re_s], 1).astype(jnp.bfloat16)
            halfway = exchange(halfway.reshape(group, part, 2 * part), same_frequency, group, 1)
            halfway = halfway.reshape(group, part, 2, part).transpose(2, 1, 0, 3)
            re_c, im_c, re_s, im_s = rows_times(halfway.reshape(2, part, extent), cosine, sine)
            model = jnp.stack([re_c - im_s, re_s + im_c]).astype(jnp.bfloat16)
            re_r, im_r, re_i, im_i = rows_times(model, data_re, data_im)
            prod_re, prod_im = re_r - im_i, re_i + im_r
            misfit = (
                rows.astype(jnp.float32)
                - model.astype(jnp.float32)
                + jnp.stack(
                    [
                        prod_re * wave_re - prod_im * wave_im,
                        prod_re * wave_im + prod_im * wave_re,
                    ]
                )
            )
        squares = jnp.sum(misfit * misfit)
        misfit_half = misfit.astype(jnp.bfloat16)
        re_r, im_r, re_i, im_i = rows_times(misfit_half, data_re, data_im, "mr,kr->mk")
        back_re, back_im = re_r + im_i, im_r - re_i
        scaled = jnp.stack(
            [back_re * wave_re + back_im * wave_im, back_im * wave_re - back_re * wave_im]
        )
        grad_half = (misfit_half.astype(jnp.float32) - scaled).astype(jnp.bfloat16)
        re_c, im_c, re_s, im_s = rows_times(grad_half, cosine, sine)
        turned = jnp.stack([re_c + im_s, im_c - re_s]).astype(jnp.bfloat16)
        turned = turned.reshape(2, part, group, part).transpose(2, 0, 1, 3)
        turned = exchange(turned, same_frequency, group, 2)
        turned = turned.transpose(0, 2, 1, 3).reshape(extent, 2 * part)
        re_c, im_c, re_s, im_s = times_columns(turned)
        trial_re = coeffs_re + step_length * (re_c + im_s)
        trial_im = coeffs_im + step_length * (im_c - re_s)
        magnitude = jnp.sqrt(trial_re * trial_re + trial_im * trial_im)
        upper = lax.broadcasted_iota(jnp.int32, (8, 128), 0) < 4
        tile = jnp.where(upper, jnp.max(magnitude), squares)
        gathered = exchange(tile, everyone, nsrc * nrcv, 3, whole=True)
        gathered = gathered.reshape(nz, nf, nrcv, 8, 128)
        norm_list.append(jnp.sqrt(jnp.sum(gathered[:, :, :, 4, 0], axis=(0, 2))))
        peaks = jnp.max(gathered[:, :, :, 0, 0], axis=(0, 2))
        level = shrink_fraction * lax.dynamic_slice_in_dim(peaks, f, 1, 0)[0]
        factor = jnp.maximum(1.0 - level / jnp.maximum(magnitude, level), 0.0)
        coeffs_re, coeffs_im = trial_re * factor, trial_im * factor
    stacked = jnp.concatenate([coeffs_re, coeffs_im], 1).astype(jnp.bfloat16)
    spread = exchange(stacked.reshape(nsrc, extent // nsrc, 2 * part), same_column, nsrc, 4)
    spread = spread.reshape(nz, nf, extent // nsrc, 2, part).transpose(1, 3, 2, 0, 4)
    coeffs = spread.reshape(traces.shape).astype(jnp.float32)
    return (coeffs, jnp.stack(norm_list))


def solution(mesh):
    in_specs = (P(None, None, "src", "rcv"), P())
    out_specs = (P(None, None, "src", "rcv"), P())
    body = functools.partial(per_device, mesh.shape["src"], mesh.shape["rcv"])
    return jax.shard_map(body, mesh=mesh, in_specs=in_specs, out_specs=out_specs, check_vma=False)
```

```python
import functools
import math

import jax
import jax.numpy as jnp
from jax import lax
from jax.experimental import pallas as pl
from jax.experimental.pallas import tpu as pltpu
from jax.sharding import PartitionSpec as P

ITERS = 2
CORES = 2
MESH = pl.DeviceIdType.MESH

step_length = 0.4
shrink_fraction = 0.2


def exchange_kernel(members, whole, x_ref, out_ref, send_sem, recv_sem, own_sem):
    count, me, device = members()
    barrier = pltpu.get_barrier_semaphore()
    for step in range(1, count):
        pl.semaphore_signal(
            barrier, inc=1, device_id=device(lax.rem(me + step, count)), device_id_type=MESH
        )
    pl.semaphore_wait(barrier, count - 1)
    own = pltpu.make_async_copy(x_ref if whole else x_ref.at[me], out_ref.at[me], own_sem)
    own.start()
    sends = []
    for step in range(1, count):
        peer = lax.rem(me + step, count)
        copy = pltpu.make_async_remote_copy(
            src_ref=x_ref if whole else x_ref.at[peer],
            dst_ref=out_ref.at[me],
            send_sem=send_sem.at[step],
            recv_sem=recv_sem.at[step],
            device_id=device(peer),
            device_id_type=MESH,
        )
        copy.start()
        sends.append(copy)
    own.wait()
    for step in range(1, count):
        origin = lax.rem(me - step + count, count)
        pltpu.make_async_remote_copy(
            src_ref=out_ref.at[origin],
            dst_ref=out_ref.at[origin],
            send_sem=send_sem.at[step],
            recv_sem=recv_sem.at[step],
            device_id=device(origin),
            device_id_type=MESH,
        ).wait_recv()
    for copy in sends:
        copy.wait_send()


def exchange(x, members, count, ident, whole=False):
    shape = (count,) + x.shape if whole else x.shape
    return pl.pallas_call(
        functools.partial(exchange_kernel, members, whole),
        out_shape=jax.ShapeDtypeStruct(shape, x.dtype),
        in_specs=[pl.BlockSpec(memory_space=pltpu.VMEM)],
        out_specs=pl.BlockSpec(memory_space=pltpu.VMEM),
        scratch_shapes=[
            pltpu.SemaphoreType.DMA((count,)),
            pltpu.SemaphoreType.DMA((count,)),
            pltpu.SemaphoreType.DMA,
        ],
        compiler_params=pltpu.CompilerParams(collective_id=ident, has_side_effects=True),
    )(x)


def gather_kernel(nz, ny, nf, x_ref, out_ref, own_sem, swap_sem, link_sem, core_sem, send_sem):
    src, rcv = lax.axis_index("src"), lax.axis_index("rcv")
    z, f = src // nf, lax.rem(src, nf)
    y, c = rcv // CORES, lax.rem(rcv, CORES)
    height, width = x_ref.shape[2], x_ref.shape[3]

    def device(zz, ff, yy, cc):
        return (zz * nf + ff, yy * CORES + cc)

    def block(zz, ff, yy, cc):
        top = pl.multiple_of((zz * nf + ff) * height, height)
        left = pl.multiple_of((yy * CORES + cc) * width, width)
        return out_ref.at[:, pl.ds(top, height), pl.ds(left, width)]

    z_peers = [lax.rem(z + d, nz) for d in range(1, nz)]
    y_peers = [lax.rem(y + e, ny) for e in range(1, ny)]
    f_peers = [lax.rem(f + g, nf) for g in range(1, nf)]
    other = 1 - c

    barrier = pltpu.get_barrier_semaphore()
    targets = [device(zz, f, y, c) for zz in z_peers]
    targets += [device(z, f, yy, c) for yy in y_peers]
    targets += [device(z, ff, y, c) for ff in f_peers]
    targets += [device(z, f, y, other)]
    for target in targets:
        pl.semaphore_signal(barrier, inc=1, device_id=target, device_id_type=MESH)
    pl.semaphore_wait(barrier, len(targets))

    sends = []

    def push(source, place, semaphore, target):
        copy = pltpu.make_async_remote_copy(
            src_ref=source,
            dst_ref=place,
            send_sem=send_sem.at[len(sends)],
            recv_sem=semaphore,
            device_id=target,
            device_id_type=MESH,
        )
        copy.start()
        sends.append(copy)

    def await_block(place, semaphore):
        pltpu.make_async_remote_copy(
            src_ref=place,
            dst_ref=place,
            send_sem=send_sem.at[0],
            recv_sem=semaphore,
            device_id=device(z, f, y, other),
            device_id_type=MESH,
        ).wait_recv()

    def across(zz, ff, yy):
        here = block(zz, ff, yy, c)
        push(here, here, core_sem.at[zz, ff, yy], device(z, f, y, other))

    def along_z(ff, yy):
        here = block(z, ff, yy, c)
        for zz in z_peers:
            push(here, here, link_sem.at[z, ff, yy], device(zz, f, y, c))

    def along_y(zz, ff):
        here = block(zz, ff, y, c)
        for yy in y_peers:
            push(here, here, link_sem.at[zz, ff, y], device(z, f, yy, c))

    for step, ff in enumerate(f_peers):
        push(x_ref.at[ff], block(z, f, y, c), swap_sem.at[step], device(z, ff, y, c))
    own = pltpu.make_async_copy(x_ref.at[f], block(z, f, y, c), own_sem)
    own.start()
    own.wait()
    for step in range(nf - 1):
        origin = lax.rem(f - 1 - step + nf, nf)
        await_block(block(z, origin, y, c), swap_sem.at[step])

    for ff in range(nf):
        if ff % 2 == 0:
            along_z(ff, y)
        else:
            along_y(z, ff)
    for ff in range(nf):
        across(z, ff, y)
    for ff in range(nf):
        if ff % 2 == 0:
            along_y(z, ff)
        else:
            along_z(ff, y)
    for ff in range(1, nf, 2):
        for yy in y_peers:
            await_block(block(z, ff, yy, c), link_sem.at[z, ff, yy])
            along_z(ff, yy)
            across(z, ff, yy)
    for ff in range(0, nf, 2):
        for zz in z_peers:
            await_block(block(zz, ff, y, c), link_sem.at[zz, ff, y])
            along_y(zz, ff)
            across(zz, ff, y)
    for ff in range(0, nf, 2):
        for yy in y_peers:
            await_block(block(z, ff, yy, c), link_sem.at[z, ff, yy])
            across(z, ff, yy)
    for ff in range(1, nf, 2):
        for zz in z_peers:
            await_block(block(zz, ff, y, c), link_sem.at[zz, ff, y])
            across(zz, ff, y)
    for ff in range(nf):
        for zz in z_peers:
            for yy in y_peers:
                await_block(block(zz, ff, yy, c), link_sem.at[zz, ff, yy])
                across(zz, ff, yy)
    for ff in range(nf):
        for zz in range(nz):
            for yy in range(ny):
                await_block(block(zz, ff, yy, other), core_sem.at[zz, ff, yy])
    for copy in sends:
        copy.wait_send()


def gather(traces, nz, ny, nf, extent):
    even, odd = (nf + 1) // 2, nf // 2
    total = (nf - 1) + nf * nz * ny
    total += even * ((nz - 1) + nz * (ny - 1)) + odd * ((ny - 1) + ny * (nz - 1))
    return pl.pallas_call(
        functools.partial(gather_kernel, nz, ny, nf),
        out_shape=jax.ShapeDtypeStruct((2, extent, extent), traces.dtype),
        in_specs=[pl.BlockSpec(memory_space=pltpu.VMEM)],
        out_specs=pl.BlockSpec(memory_space=pl.ANY),
        scratch_shapes=[
            pltpu.SemaphoreType.DMA,
            pltpu.SemaphoreType.DMA((nf,)),
            pltpu.SemaphoreType.DMA((nz, nf, ny)),
            pltpu.SemaphoreType.DMA((nz, nf, ny)),
            pltpu.SemaphoreType.DMA((total + nf * (nz + ny),)),
        ],
        compiler_params=pltpu.CompilerParams(collective_id=0, has_side_effects=True),
    )(traces)


def tables(extent):
    low = 1 << (extent.bit_length() // 2)
    while extent % low:
        low //= 2
    row = jnp.arange(extent, dtype=jnp.int32)

    def parts(column, scale):
        phase = row[:, None] * column[None, :] % extent
        angle = phase.astype(jnp.float32) * (2.0 * math.pi / extent)
        return lax.optimization_barrier((jnp.cos(angle) * scale, jnp.sin(angle) * scale))

    cos_low, sin_low = parts(jnp.arange(low, dtype=jnp.int32), 1.0)
    cos_high, sin_high = parts(
        jnp.arange(extent // low, dtype=jnp.int32) * low, 1.0 / math.sqrt(extent)
    )
    cos_high, sin_high = jnp.repeat(cos_high, low, 1), jnp.repeat(sin_high, low, 1)
    cos_low = jnp.tile(cos_low, (1, extent // low))
    sin_low = jnp.tile(sin_low, (1, extent // low))
    cosine = (cos_high * cos_low - sin_high * sin_low).astype(jnp.bfloat16)
    sine = (sin_high * cos_low + cos_high * sin_low).astype(jnp.bfloat16)
    return lax.optimization_barrier((cosine, sine))


def dot(left, right, pattern="mn,nc->mc"):
    return jnp.einsum(pattern, left, right, preferred_element_type=jnp.float32)


def per_device(nsrc, nrcv, traces, wavelet):
    nf, extent = traces.shape[0], traces.shape[2] * nsrc
    nz, ny = nsrc // nf, nrcv // CORES
    group = nz * nrcv
    part = extent // group
    src, rcv = lax.axis_index("src"), lax.axis_index("rcv")
    f = lax.rem(src, nf)
    place = rcv * nz + src // nf

    def same_frequency():
        src, rcv = lax.axis_index("src"), lax.axis_index("rcv")
        f = lax.rem(src, nf)
        return group, rcv * nz + src // nf, lambda i: (lax.rem(i, nz) * nf + f, i // nz)

    def same_column():
        rcv = lax.axis_index("rcv")
        return nsrc, lax.axis_index("src"), lambda i: (i, rcv)

    def everyone():
        me = lax.axis_index("src") * nrcv + lax.axis_index("rcv")
        return nsrc * nrcv, me, lambda i: (i // nrcv, lax.rem(i, nrcv))

    root_scale = 1.0 / math.sqrt(extent)
    wave = lax.dynamic_slice_in_dim(wavelet, f, 1, 0)[0] * root_scale
    wave_re, wave_im = wave[0], wave[1]

    cosine, sine = tables(extent)
    data = gather(traces, nz, ny, nf, extent)
    data_re, data_im = data[0], data[1]
    rows = lax.dynamic_slice_in_dim(data, place * part, part, 1)

    def rows_times(left, first, second, pattern="mn,nc->mc"):
        stacked = left.reshape(2 * part, extent)
        a = dot(stacked, first, pattern).reshape(2, part, extent)
        b = dot(stacked, second, pattern).reshape(2, part, extent)
        return a[0], a[1], b[0], b[1]

    def times_columns(right):
        a, b = dot(cosine, right), dot(sine, right)
        return a[:, :part], a[:, part:], b[:, :part], b[:, part:]

    coeffs_re = jnp.zeros((extent, part), jnp.float32)
    coeffs_im = coeffs_re
    norm_list = []
    for iteration in range(ITERS):
        if iteration == 0:
            misfit = rows.astype(jnp.float32)
        else:
            stacked = jnp.concatenate([coeffs_re, coeffs_im], 1).astype(jnp.bfloat16)
            re_c, im_c, re_s, im_s = times_columns(stacked)
            halfway = jnp.concatenate([re_c - im_s, im_c + re_s], 1).astype(jnp.bfloat16)
            halfway = exchange(halfway.reshape(group, part, 2 * part), same_frequency, group, 1)
            halfway = halfway.reshape(group, part, 2, part).transpose(2, 1, 0, 3)
            re_c, im_c, re_s, im_s = rows_times(halfway.reshape(2, part, extent), cosine, sine)
            model = jnp.stack([re_c - im_s, re_s + im_c]).astype(jnp.bfloat16)
            re_r, im_r, re_i, im_i = rows_times(model, data_re, data_im)
            prod_re, prod_im = re_r - im_i, re_i + im_r
            misfit = (
                rows.astype(jnp.float32)
                - model.astype(jnp.float32)
                + jnp.stack(
                    [
                        prod_re * wave_re - prod_im * wave_im,
                        prod_re * wave_im + prod_im * wave_re,
                    ]
                )
            )
        squares = jnp.sum(misfit * misfit)
        misfit_half = misfit.astype(jnp.bfloat16)
        re_r, im_r, re_i, im_i = rows_times(misfit_half, data_re, data_im, "mr,kr->mk")
        back_re, back_im = re_r + im_i, im_r - re_i
        scaled = jnp.stack(
            [back_re * wave_re + back_im * wave_im, back_im * wave_re - back_re * wave_im]
        )
        grad_half = (misfit_half.astype(jnp.float32) - scaled).astype(jnp.bfloat16)
        re_c, im_c, re_s, im_s = rows_times(grad_half, cosine, sine)
        turned = jnp.stack([re_c + im_s, im_c - re_s]).astype(jnp.bfloat16)
        turned = turned.reshape(2, part, group, part).transpose(2, 0, 1, 3)
        turned = exchange(turned, same_frequency, group, 2)
        turned = turned.transpose(0, 2, 1, 3).reshape(extent, 2 * part)
        re_c, im_c, re_s, im_s = times_columns(turned)
        trial_re = coeffs_re + step_length * (re_c + im_s)
        trial_im = coeffs_im + step_length * (im_c - re_s)
        magnitude = jnp.sqrt(trial_re * trial_re + trial_im * trial_im)
        upper = lax.broadcasted_iota(jnp.int32, (8, 128), 0) < 4
        tile = jnp.where(upper, jnp.max(magnitude), squares)
        gathered = exchange(tile, everyone, nsrc * nrcv, 3, whole=True)
        gathered = gathered.reshape(nz, nf, nrcv, 8, 128)
        norm_list.append(jnp.sqrt(jnp.sum(gathered[:, :, :, 4, 0], axis=(0, 2))))
        peaks = jnp.max(gathered[:, :, :, 0, 0], axis=(0, 2))
        level = shrink_fraction * lax.dynamic_slice_in_dim(peaks, f, 1, 0)[0]
        factor = jnp.maximum(1.0 - level / jnp.maximum(magnitude, level), 0.0)
        coeffs_re, coeffs_im = trial_re * factor, trial_im * factor
    stacked = jnp.concatenate([coeffs_re, coeffs_im], 1).astype(jnp.bfloat16)
    spread = exchange(stacked.reshape(nsrc, extent // nsrc, 2 * part), same_column, nsrc, 4)
    spread = spread.reshape(nz, nf, extent // nsrc, 2, part).transpose(1, 3, 2, 0, 4)
    coeffs = spread.reshape(traces.shape).astype(jnp.float32)
    return (coeffs, jnp.stack(norm_list))


def solution(mesh):
    in_specs = (P(None, None, "src", "rcv"), P())
    out_specs = (P(None, None, "src", "rcv"), P())
    body = functools.partial(per_device, mesh.shape["src"], mesh.shape["rcv"])
    return jax.shard_map(body, mesh=mesh, in_specs=in_specs, out_specs=out_specs, check_vma=False)
```
